32 devices in a mesh: seq: 8 (over z, y), head: 4 (over x, core).
Axes of the slice: x: 2, y: 2, z: 4, core: 2. Of those that a mesh axis runs over, the one named last changes fastest.
Arguments:
- queries: bfloat16 [2048, 8192], P('seq', 'head'), may hold values from -40 to 40
- key_rows: bfloat16 [2048, 8192], P('seq', 'head'), may hold values from -20 to 20
- value_rows: bfloat16 [2048, 8192], P('seq', 'head'), may hold values from -8 to 8
Outputs:
- attended: bfloat16 [2048, 8192], P('seq', 'head')
The draws below stay inside these ranges and needn't reach their ends.
All inputs are finite; a program needn't handle non-finite values.
Results may differ from the reference program's by a relative error of at most 0.0043.
Values may be sent and summed in bfloat16 or wider, within the bound.
A program may use at most 128 MiB of HBM per device.

```python
import math
from functools import reduce
import jax
import jax.numpy as jnp
from jax import lax

HEADS = 64
HEAD_DIM = 128
BLOCK = 128
POOL = 64
MID_REACH = 3
FAR_REACH = 9
TOKENS = 2048


def rough_field(folded, rows_total):
    return jax.random.truncated_normal(folded, -4.0, 4.0, (rows_total, HEADS * HEAD_DIM), jnp.float32)


def group_field(folded):
    group_part = jax.random.truncated_normal(folded, -4.0, 4.0, (TOKENS // POOL, HEADS * HEAD_DIM), jnp.float32)
    return jnp.repeat(group_part, POOL, axis=0)


def paired_keys(key):
    folded = jax.random.fold_in(key, 11)
    drawn = 3.0 * rough_field(jax.random.fold_in(folded, 1), TOKENS) + 1.5 * group_field(jax.random.fold_in(folded, 2))
    return drawn


def draw_key_rows(key, part):
    return paired_keys(key).astype(jnp.bfloat16)


def draw_queries(key, part):
    drawn = rough_field(jax.random.fold_in(key, 23), TOKENS)
    return drawn.astype(jnp.bfloat16)


def draw_value_rows(key, part):
    folded = jax.random.fold_in(key, 31)
    drawn = rough_field(jax.random.fold_in(folded, 1), TOKENS) + group_field(jax.random.fold_in(folded, 2))
    return drawn.astype(jnp.bfloat16)


def setup_inputs(seed: int = 0) -> dict:
    key_list = jax.random.split(jax.random.key(seed), 4)
    return {
        "queries": draw_queries(jax.random.fold_in(key_list[3], 71), 0),
        "key_rows": draw_key_rows(jax.random.fold_in(key_list[3], 71), 0),
        "value_rows": draw_value_rows(jax.random.fold_in(key_list[3], 71), 0),
    }


def pool_pairs(source):
    paired = source.astype(jnp.float32).reshape(source.shape[0] // 2, 2, source.shape[1])
    return (0.5 * (paired[:, 0] + paired[:, 1])).astype(jnp.bfloat16)

def pool_groups(source, group_rows):
    grouped = source.astype(jnp.float32).reshape(source.shape[0] // group_rows, group_rows, source.shape[1])
    return lax.optimization_barrier(jnp.mean(grouped, axis=1)).astype(jnp.bfloat16)

def padded(source, margin):
    return jnp.pad(source, ((margin, margin), (0, 0)))

def as_heads(source):
    return source.astype(jnp.float32).reshape(source.shape[0], HEADS, HEAD_DIM)

def reference(queries, key_rows, value_rows):
    score_scale = 1.0 / math.sqrt(HEAD_DIM)
    key_two = pool_pairs(key_rows)
    value_two = pool_pairs(value_rows)
    key_four = pool_pairs(key_two)
    value_four = pool_pairs(value_two)
    key_coarse = pool_groups(key_four, POOL // 4)
    value_coarse = pool_groups(value_four, POOL // 4)
    half_rows = BLOCK // 2
    quarter = BLOCK // 4
    blocks_all = TOKENS // BLOCK
    fine_pads = (padded(key_rows, BLOCK), padded(value_rows, BLOCK))
    mid_pads = (padded(key_two, MID_REACH * half_rows), padded(value_two, MID_REACH * half_rows))
    far_pads = (padded(key_four, FAR_REACH * quarter), padded(value_four, FAR_REACH * quarter))
    coarse_block = POOL * jnp.arange(TOKENS // POOL, dtype=jnp.int32) // BLOCK
    fine_span = 3 * BLOCK
    mid_span = (2 * MID_REACH + 1) * half_rows
    far_span = (2 * FAR_REACH + 1) * quarter

    def window(pads, anchor, span):
        return (lax.dynamic_slice_in_dim(pads[0], anchor, span, 0), lax.dynamic_slice_in_dim(pads[1], anchor, span, 0))

    def one_block(block_index):
        query_rows = as_heads(lax.dynamic_slice_in_dim(queries, block_index * BLOCK, BLOCK, 0))
        fine_pair = window(fine_pads, block_index * BLOCK, fine_span)
        mid_pair = window(mid_pads, block_index * half_rows, mid_span)
        far_pair = window(far_pads, block_index * quarter, far_span)
        fine_block = block_index - 1 + jnp.arange(fine_span, dtype=jnp.int32) // BLOCK
        mid_block = block_index - MID_REACH + jnp.arange(mid_span, dtype=jnp.int32) // half_rows
        far_block = block_index - FAR_REACH + jnp.arange(far_span, dtype=jnp.int32) // quarter
        level_list = [(fine_pair, fine_block, 0, 1, 0.0), (mid_pair, mid_block, 2, MID_REACH, math.log(2.0)), (far_pair, far_block, MID_REACH + 1, FAR_REACH, math.log(4.0)), ((key_coarse, value_coarse), coarse_block, FAR_REACH + 1, blocks_all, math.log(POOL))]
        score_list = []
        for pair_rows, atom_block, lowest, highest, log_size in level_list:
            gap_blocks = jnp.abs(atom_block - block_index)
            allowed = (atom_block >= 0) & (atom_block < blocks_all) & (gap_blocks >= lowest) & (gap_blocks <= highest)
            scores = jnp.einsum('qhe,khe->hqk', query_rows, as_heads(pair_rows[0])) * score_scale + log_size
            score_list.append(jnp.where(allowed[None, None, :], scores, -jnp.inf))
        row_top = reduce(jnp.maximum, [lax.optimization_barrier(jnp.max(scores, axis=2)) for scores in score_list])
        denominator = jnp.zeros((HEADS, BLOCK), jnp.float32)
        weighted = jnp.zeros((BLOCK, HEADS, HEAD_DIM), jnp.float32)
        for scores, level_item in zip(score_list, level_list):
            exp_terms = jnp.exp(scores - row_top[:, :, None])
            denominator = denominator + lax.optimization_barrier(jnp.sum(exp_terms, axis=2))
            rounded = lax.optimization_barrier(exp_terms.astype(jnp.bfloat16))
            weighted = weighted + jnp.einsum('hqk,khe->qhe', rounded.astype(jnp.float32), as_heads(level_item[0][1]))
        result = weighted / jnp.transpose(denominator)[:, :, None]
        return result.reshape(BLOCK, HEADS * HEAD_DIM).astype(jnp.bfloat16)
    blocks = lax.map(one_block, jnp.arange(blocks_all, dtype=jnp.int32))
    return blocks.reshape(TOKENS, HEADS * HEAD_DIM)
```

```python
import functools
import math

import jax
import jax.numpy as jnp
from jax import lax
from jax.experimental import pallas as pl
from jax.experimental.pallas import tpu as pltpu
from jax.sharding import PartitionSpec as P

HEAD_DIM = 128
BLOCK = 128
POOL = 64
MID_REACH = 3
FAR_REACH = 9

HALF = BLOCK // 2
QUARTER = BLOCK // 4
GROUP_BLOCKS = 4
GROUP_ROWS = GROUP_BLOCKS * BLOCK
COARSE_SLOT = 16
COARSE_USED = GROUP_ROWS // POOL

FINE_LOW, FINE_BLOCKS = -1, GROUP_BLOCKS + 2
MID_LOW, MID_BLOCKS = -MID_REACH, GROUP_BLOCKS + 2 * MID_REACH
FAR_LOW, FAR_BLOCKS = -FAR_REACH, GROUP_BLOCKS + 2 * FAR_REACH

KIND_K, KIND_V, KIND_Q, KIND_O = 0, 1, 2, 3
ROUTES = (
    (4, 1, "fine", 3, 1, -1),
    (5, -1, "fine", 0, 1, 4),
    (6, 1, "mid", 1, 2, -3),
    (7, -1, "mid", 1, 2, 5),
    (8, 2, "far", 0, 4, -8),
    (9, -2, "far", 0, 4, 8),
    (10, 1, "far", 0, 1, -4),
    (11, -1, "far", 3, 1, 7),
    (12, 3, "far", 3, 1, -9),
    (13, -3, "far", 0, 1, 12),
)
KINDS = 14
MESH = pl.DeviceIdType.MESH


def pool_matrix(out_rows, in_rows, group_rows, used_rows=None):
    row = lax.broadcasted_iota(jnp.int32, (out_rows, in_rows), 0)
    col = lax.broadcasted_iota(jnp.int32, (out_rows, in_rows), 1)
    return jnp.where(col // group_rows == row, 1.0 / group_rows, 0.0).astype(jnp.bfloat16)


def pooled(source, out_rows, group_rows):
    weights = pool_matrix(out_rows, source.shape[0], group_rows)
    return jnp.dot(weights, source, preferred_element_type=jnp.float32).astype(jnp.bfloat16)


def kernel(
    groups, q_ref, k_ref, v_ref, o_ref,
    q_rows, fine, mid, far, coarse, out_rows, out_back, bias,
    send, recv, coarse_send, coarse_recv,
):
    me = lax.axis_index("seq")
    group = me // 2
    parity = me % 2
    partner = me + 1 - 2 * parity
    rows_dev = q_ref.shape[0]
    chunks = q_rows.shape[0]
    half_cols = chunks * HEAD_DIM
    own_first = pl.multiple_of(parity * rows_dev, rows_dev)
    other_first = pl.multiple_of((1 - parity) * rows_dev, rows_dev)
    levels = {"fine": (fine, BLOCK, FINE_LOW), "mid": (mid, HALF, MID_LOW), "far": (far, QUARTER, FAR_LOW)}

    def own_cols(chunk):
        return pl.ds(pl.multiple_of(parity * half_cols + chunk * HEAD_DIM, HEAD_DIM), HEAD_DIM)

    def other_cols(chunk):
        return pl.ds(pl.multiple_of((1 - parity) * half_cols + chunk * HEAD_DIM, HEAD_DIM), HEAD_DIM)

    def remote(src, dst, kind, chunk, target):
        return pltpu.make_async_remote_copy(
            src_ref=src, dst_ref=dst, send_sem=send.at[chunk, kind], recv_sem=recv.at[chunk, kind],
            device_id={"seq": target}, device_id_type=MESH,
        )

    def exchange(kind, chunk):
        if kind == KIND_Q:
            return remote(
                q_ref.at[:, other_cols(chunk)], q_rows.at[chunk, pl.ds(own_first, rows_dev)],
                kind, chunk, partner,
            )
        if kind == KIND_O:
            return remote(
                out_rows.at[chunk, pl.ds(other_first, rows_dev)], out_back.at[chunk], kind, chunk, partner
            )
        source = k_ref if kind == KIND_K else v_ref
        return remote(
            source.at[:, other_cols(chunk)], fine.at[chunk, kind, pl.ds(BLOCK + own_first, rows_dev)],
            kind, chunk, partner,
        )

    def routed(route, chunk):
        kind, offset, level, first, count, landing = route
        window, unit, low = levels[level]
        return remote(
            window.at[chunk, :, pl.ds((first - low) * unit, count * unit)],
            window.at[chunk, :, pl.ds((landing - low) * unit, count * unit)],
            kind, chunk, me + 2 * offset,
        )

    def coarse_copy(chunk, step):
        target = lax.rem(group + step, groups) * 2 + parity
        slot = pl.ds(pl.multiple_of(group * COARSE_SLOT, COARSE_SLOT), COARSE_SLOT)
        return pltpu.make_async_remote_copy(
            src_ref=coarse.at[chunk, :, slot], dst_ref=coarse.at[chunk, :, slot],
            send_sem=coarse_send.at[chunk, step], recv_sem=coarse_recv.at[chunk, step],
            device_id={"seq": target}, device_id_type=MESH,
        )

    def inside(offset):
        return (group + offset >= 0) & (group + offset < groups)

    barrier = pltpu.get_barrier_semaphore()
    pl.semaphore_signal(barrier, inc=1, device_id={"seq": partner}, device_id_type=MESH)

    @pl.loop(1, groups)
    def _(step):
        target = lax.rem(group + step, groups) * 2 + parity
        pl.semaphore_signal(barrier, inc=1, device_id={"seq": target}, device_id_type=MESH)

    pl.semaphore_wait(barrier, groups)

    @pl.loop(0, chunks)
    def _(chunk):
        exchange(KIND_K, chunk).start()
        exchange(KIND_V, chunk).start()

    @pl.loop(0, chunks)
    def _(chunk):
        exchange(KIND_Q, chunk).start()

    for _, offset, level, _, count, landing in ROUTES:
        window, unit, low = levels[level]

        @pl.when(jnp.logical_not(inside(-offset)))
        def _():
            @pl.loop(0, chunks)
            def _(chunk):
                window[chunk, :, pl.ds((landing - low) * unit, count * unit)] = jnp.zeros(
                    (2, count * unit, HEAD_DIM), jnp.bfloat16
                )

    atoms = bias.shape[1]
    total_blocks = groups * GROUP_BLOCKS
    place = lax.broadcasted_iota(jnp.int32, (1, atoms), 1)
    windows_end = 8 * BLOCK
    for block in range(GROUP_BLOCKS):
        rel = jnp.where(
            place < 384,
            block - 1 + place // BLOCK,
            jnp.where(
                place < 512,
                block - 3 + (place - 384) // HALF,
                jnp.where(
                    place < 640,
                    block + 2 + (place - 512) // HALF,
                    jnp.where(
                        place < 832,
                        block - 9 + (place - 640) // QUARTER,
                        block + 4 + (place - 832) // QUARTER,
                    ),
                ),
            ),
        )
        here = group * GROUP_BLOCKS + rel
        held = (here >= 0) & (here < total_blocks)
        late = place - windows_end
        slot_row = late % COARSE_SLOT
        coarse_block = late // COARSE_SLOT * GROUP_BLOCKS + slot_row * POOL // BLOCK
        apart = jnp.abs(coarse_block - (group * GROUP_BLOCKS + block)) > FAR_REACH
        allowed = ((place < windows_end) & held) | (
            (place >= windows_end) & (slot_row < COARSE_USED) & apart
        )
        log_size = jnp.where(
            place < 384, 0.0, jnp.where(place < 640, 1.0, jnp.where(place < windows_end, 2.0, math.log2(POOL)))
        )
        bias[pl.ds(block, 1), :] = jnp.where(allowed, log_size, -jnp.inf)

    @pl.loop(0, chunks)
    def _(chunk):
        own = pl.ds(BLOCK + own_first, rows_dev)
        fine[chunk, 0, own] = k_ref[:, own_cols(chunk)]
        fine[chunk, 1, own] = v_ref[:, own_cols(chunk)]
        q_rows[chunk, pl.ds(own_first, rows_dev)] = q_ref[:, own_cols(chunk)]
        exchange(KIND_K, chunk).wait_recv()
        exchange(KIND_V, chunk).wait_recv()
        for route in ROUTES[:2]:
            @pl.when(inside(route[1]))
            def _():
                routed(route, chunk).start()
        slot = pl.ds(pl.multiple_of(group * COARSE_SLOT, COARSE_SLOT), COARSE_SLOT)
        for side in range(2):
            rows = fine[chunk, side, BLOCK : BLOCK + GROUP_ROWS]
            twos = pooled(rows, GROUP_ROWS // 2, 2)
            fours = pooled(twos, GROUP_ROWS // 4, 2)
            mid[chunk, side, -MID_LOW * HALF : (GROUP_BLOCKS - MID_LOW) * HALF] = twos
            far[chunk, side, -FAR_LOW * QUARTER : (GROUP_BLOCKS - FAR_LOW) * QUARTER] = fours
            coarse[chunk, side, slot] = pooled(fours, COARSE_SLOT, POOL // 4)
        for route in ROUTES[2:]:
            @pl.when(inside(route[1]))
            def _():
                routed(route, chunk).start()

        @pl.loop(1, groups)
        def _(step):
            coarse_copy(chunk, step).start()

    scale = math.log2(math.e) / math.sqrt(HEAD_DIM)

    @pl.loop(0, chunks)
    def _(chunk):
        exchange(KIND_Q, chunk).wait_recv()
        for route in ROUTES:
            @pl.when(inside(-route[1]))
            def _():
                routed(route, chunk).wait_recv()

        @pl.loop(1, groups)
        def _(step):
            origin = pl.ds(
                pl.multiple_of(lax.rem(group - step + groups, groups) * COARSE_SLOT, COARSE_SLOT), COARSE_SLOT
            )
            pltpu.make_async_remote_copy(
                src_ref=coarse.at[chunk, :, origin], dst_ref=coarse.at[chunk, :, origin],
                send_sem=coarse_send.at[chunk, step], recv_sem=coarse_recv.at[chunk, step],
                device_id={"seq": partner}, device_id_type=MESH,
            ).wait_recv()

        for side in range(2):
            mid[chunk, side, 2 * HALF : 3 * HALF] = pooled(fine[chunk, side, :BLOCK], HALF, 2)
            mid[chunk, side, 7 * HALF : 8 * HALF] = pooled(fine[chunk, side, 5 * BLOCK :], HALF, 2)
            far[chunk, side, 6 * QUARTER : 9 * QUARTER] = pooled(
                mid[chunk, side, : 3 * HALF], 3 * QUARTER, 2
            )
            far[chunk, side, 13 * QUARTER : 16 * QUARTER] = pooled(
                mid[chunk, side, 7 * HALF :], 3 * QUARTER, 2
            )

        for block in range(GROUP_BLOCKS):
            def atom_rows(side):
                return jnp.concatenate(
                    [
                        fine[chunk, side, block * BLOCK : (block + 3) * BLOCK],
                        mid[chunk, side, block * HALF : (block + 2) * HALF],
                        mid[chunk, side, (block + 5) * HALF : (block + 7) * HALF],
                        far[chunk, side, block * QUARTER : (block + 6) * QUARTER],
                        far[chunk, side, (block + 13) * QUARTER : (block + 19) * QUARTER],
                        coarse[chunk, side],
                    ],
                    axis=0,
                )

            scores = lax.dot_general(
                q_rows[chunk, block * BLOCK : (block + 1) * BLOCK], atom_rows(0),
                (((1,), (1,)), ((), ())), preferred_element_type=jnp.float32,
            ) * scale + bias[pl.ds(block, 1), :]
            row_top = jnp.max(scores, axis=1, keepdims=True)
            exp_terms = jnp.exp2(scores - row_top)
            denominator = jnp.sum(exp_terms, axis=1, keepdims=True)
            weighted = jnp.dot(
                exp_terms.astype(jnp.bfloat16), atom_rows(1), preferred_element_type=jnp.float32
            )
            out_rows[chunk, block * BLOCK : (block + 1) * BLOCK] = (weighted / denominator).astype(
                jnp.bfloat16
            )
        exchange(KIND_O, chunk).start()
        o_ref[:, own_cols(chunk)] = out_rows[chunk, pl.ds(own_first, rows_dev)]

    @pl.loop(0, chunks)
    def _(chunk):
        exchange(KIND_O, chunk).wait_recv()
        o_ref[:, other_cols(chunk)] = out_back[chunk]

    @pl.loop(0, chunks)
    def _(chunk):
        for kind in (KIND_K, KIND_V, KIND_Q, KIND_O):
            exchange(kind, chunk).wait_send()
        for route in ROUTES:
            @pl.when(inside(route[1]))
            def _():
                routed(route, chunk).wait_send()

        @pl.loop(1, groups)
        def _(step):
            coarse_copy(chunk, step).wait_send()


def per_device(queries, key_rows, value_rows):
    rows_dev, cols = queries.shape
    groups = lax.axis_size("seq") // 2
    chunks = cols // 2 // HEAD_DIM
    atoms = 8 * BLOCK + groups * COARSE_SLOT
    bf16 = jnp.bfloat16
    vmem = pl.BlockSpec(memory_space=pltpu.VMEM)
    return pl.pallas_call(
        functools.partial(kernel, groups),
        out_shape=jax.ShapeDtypeStruct(queries.shape, bf16),
        in_specs=[vmem] * 3,
        out_specs=vmem,
        scratch_shapes=[
            pltpu.VMEM((chunks, 2 * rows_dev, HEAD_DIM), bf16),
            pltpu.VMEM((chunks, 2, FINE_BLOCKS * BLOCK, HEAD_DIM), bf16),
            pltpu.VMEM((chunks, 2, MID_BLOCKS * HALF, HEAD_DIM), bf16),
            pltpu.VMEM((chunks, 2, FAR_BLOCKS * QUARTER, HEAD_DIM), bf16),
            pltpu.VMEM((chunks, 2, groups * COARSE_SLOT, HEAD_DIM), bf16),
            pltpu.VMEM((chunks, 2 * rows_dev, HEAD_DIM), bf16),
            pltpu.VMEM((chunks, rows_dev, HEAD_DIM), bf16),
            pltpu.VMEM((8, atoms), jnp.float32),
            pltpu.SemaphoreType.DMA((chunks, KINDS)),
            pltpu.SemaphoreType.DMA((chunks, KINDS)),
            pltpu.SemaphoreType.DMA((chunks, groups)),
            pltpu.SemaphoreType.DMA((chunks, groups)),
        ],
        compiler_params=pltpu.CompilerParams(
            collective_id=0, has_side_effects=True, vmem_limit_bytes=48 * 1024 * 1024
        ),
    )(queries, key_rows, value_rows)


def solution(mesh):
    placed = (P("seq", "head"), P("seq", "head"), P("seq", "head"))
    return jax.shard_map(
        per_device, mesh=mesh, in_specs=placed, out_specs=P("seq", "head"), check_vma=False
    )
```

```python
import functools
import math

import jax
import jax.numpy as jnp
from jax import lax
from jax.experimental import pallas as pl
from jax.experimental.pallas import tpu as pltpu
from jax.sharding import PartitionSpec as P

HEAD_DIM = 128
BLOCK = 128
POOL = 64
MID_REACH = 3
FAR_REACH = 9

HALF = BLOCK // 2
QUARTER = BLOCK // 4
GROUP_BLOCKS = 4
GROUP_ROWS = GROUP_BLOCKS * BLOCK
COARSE_SLOT = 16
COARSE_USED = GROUP_ROWS // POOL

FINE_LOW, FINE_BLOCKS = -1, GROUP_BLOCKS + 2
MID_LOW, MID_BLOCKS = -MID_REACH, GROUP_BLOCKS + 2 * MID_REACH
FAR_LOW, FAR_BLOCKS = -FAR_REACH, GROUP_BLOCKS + 2 * FAR_REACH

KIND_K, KIND_V, KIND_Q, KIND_O = 0, 1, 2, 3
FIRST_HOP = (
    (4, 1, "fine", 3, 1, -1),
    (5, -1, "fine", 0, 1, 4),
    (6, 1, "mid", 1, 2, -3),
    (7, -1, "mid", 1, 2, 5),
    (8, 1, "far", 0, 1, -4),
    (9, -1, "far", 3, 1, 7),
)
SECOND_HOP = (
    (10, 2, "far", -4, 4, -8),
    (11, -2, "far", 4, 4, 8),
)
THIRD_HOP = (
    (12, 3, "far", -5, 1, -9),
    (13, -3, "far", 8, 1, 12),
)
ROUTES = FIRST_HOP + SECOND_HOP + THIRD_HOP
RELAY_LAG, FORWARD_LAG, ATTEND_LAG = 2, 3, 4
KINDS = 14
MESH = pl.DeviceIdType.MESH


def hop_of(offset):
    return 1 if offset > 0 else -1


def pool_matrix(out_rows, in_rows, group_rows):
    row = lax.broadcasted_iota(jnp.int32, (out_rows, in_rows), 0)
    col = lax.broadcasted_iota(jnp.int32, (out_rows, in_rows), 1)
    return jnp.where(col // group_rows == row, 1.0 / group_rows, 0.0).astype(jnp.bfloat16)


def pooled(source, out_rows, group_rows):
    weights = pool_matrix(out_rows, source.shape[0], group_rows)
    return jnp.dot(weights, source, preferred_element_type=jnp.float32).astype(jnp.bfloat16)


def kernel(
    groups, q_ref, k_ref, v_ref, o_ref,
    q_rows, fine, mid, far, coarse, out_rows, bias,
    send, recv, coarse_send, coarse_recv, local,
):
    me = lax.axis_index("seq")
    group = me // 2
    parity = me % 2
    partner = me + 1 - 2 * parity
    rows_dev = q_ref.shape[0]
    chunks = q_rows.shape[0]
    half_cols = chunks * HEAD_DIM
    own_first = pl.multiple_of(parity * rows_dev, rows_dev)
    other_first = pl.multiple_of((1 - parity) * rows_dev, rows_dev)
    levels = {"fine": (fine, BLOCK, FINE_LOW), "mid": (mid, HALF, MID_LOW), "far": (far, QUARTER, FAR_LOW)}

    def own_cols(chunk):
        return pl.ds(pl.multiple_of(parity * half_cols + chunk * HEAD_DIM, HEAD_DIM), HEAD_DIM)

    def other_cols(chunk):
        return pl.ds(pl.multiple_of((1 - parity) * half_cols + chunk * HEAD_DIM, HEAD_DIM), HEAD_DIM)

    def remote(src, dst, kind, chunk, target):
        return pltpu.make_async_remote_copy(
            src_ref=src, dst_ref=dst, send_sem=send.at[chunk, kind], recv_sem=recv.at[chunk, kind],
            device_id={"seq": target}, device_id_type=MESH,
        )

    def exchange(kind, chunk):
        if kind == KIND_Q:
            return remote(
                q_ref.at[:, other_cols(chunk)], q_rows.at[chunk, pl.ds(own_first, rows_dev)],
                kind, chunk, partner,
            )
        if kind == KIND_O:
            return remote(
                out_rows.at[chunk, pl.ds(other_first, rows_dev)], o_ref.at[:, own_cols(chunk)],
                kind, chunk, partner,
            )
        source = k_ref if kind == KIND_K else v_ref
        return remote(
            source.at[:, other_cols(chunk)], fine.at[chunk, kind, pl.ds(BLOCK + own_first, rows_dev)],
            kind, chunk, partner,
        )

    def routed(route, chunk):
        kind, offset, level, first, count, landing = route
        window, unit, low = levels[level]
        return remote(
            window.at[chunk, :, pl.ds((first - low) * unit, count * unit)],
            window.at[chunk, :, pl.ds((landing - low) * unit, count * unit)],
            kind, chunk, me + 2 * hop_of(offset),
        )

    def coarse_copy(chunk, step):
        target = lax.rem(group + step, groups) * 2 + parity
        slot = pl.ds(pl.multiple_of(group * COARSE_SLOT, COARSE_SLOT), COARSE_SLOT)
        return pltpu.make_async_remote_copy(
            src_ref=coarse.at[chunk, :, slot], dst_ref=coarse.at[chunk, :, slot],
            send_sem=coarse_send.at[chunk, step], recv_sem=coarse_recv.at[chunk, step],
            device_id={"seq": target}, device_id_type=MESH,
        )

    def inside(offset):
        return (group + offset >= 0) & (group + offset < groups)

    def start_routes(routes, chunk):
        for route in routes:
            hop = hop_of(route[1])

            @pl.when(inside(hop) & inside(hop - route[1]))
            def _():
                routed(route, chunk).start()

    def await_routes(routes, chunk):
        for route in routes:
            @pl.when(inside(-route[1]))
            def _():
                routed(route, chunk).wait_recv()

    def own_copy(kind, chunk):
        if kind == KIND_Q:
            source, target = q_ref, q_rows.at[chunk, pl.ds(own_first, rows_dev)]
        else:
            source = k_ref if kind == KIND_K else v_ref
            target = fine.at[chunk, kind, pl.ds(BLOCK + own_first, rows_dev)]
        return pltpu.make_async_copy(source.at[:, own_cols(chunk)], target, local.at[chunk, kind])

    def own_result(chunk):
        return pltpu.make_async_copy(
            out_rows.at[chunk, pl.ds(own_first, rows_dev)], o_ref.at[:, own_cols(chunk)],
            local.at[chunk, KIND_O],
        )

    barrier = pltpu.get_barrier_semaphore()
    pl.semaphore_signal(barrier, inc=1, device_id={"seq": partner}, device_id_type=MESH)

    @pl.loop(1, groups)
    def _(step):
        target = lax.rem(group + step, groups) * 2 + parity
        pl.semaphore_signal(barrier, inc=1, device_id={"seq": target}, device_id_type=MESH)

    pl.semaphore_wait(barrier, groups)

    @pl.loop(0, chunks)
    def _(chunk):
        exchange(KIND_K, chunk).start()
        exchange(KIND_V, chunk).start()
        own_copy(KIND_K, chunk).start()
        own_copy(KIND_V, chunk).start()

    @pl.loop(0, chunks)
    def _(chunk):
        exchange(KIND_Q, chunk).start()
        own_copy(KIND_Q, chunk).start()

    for _, offset, level, _, count, landing in ROUTES:
        window, unit, low = levels[level]

        @pl.when(jnp.logical_not(inside(-offset)))
        def _():
            @pl.loop(0, chunks)
            def _(chunk):
                window[chunk, :, pl.ds((landing - low) * unit, count * unit)] = jnp.zeros(
                    (2, count * unit, HEAD_DIM), jnp.bfloat16
                )

    atoms = bias.shape[1]
    total_blocks = groups * GROUP_BLOCKS
    place = lax.broadcasted_iota(jnp.int32, (1, atoms), 1)
    windows_end = 8 * BLOCK
    for block in range(GROUP_BLOCKS):
        rel = jnp.where(
            place < 384,
            block - 1 + place // BLOCK,
            jnp.where(
                place < 512,
                block - 3 + (place - 384) // HALF,
                jnp.where(
                    place < 640,
                    block + 2 + (place - 512) // HALF,
                    jnp.where(
                        place < 832,
                        block - 9 + (place - 640) // QUARTER,
                        block + 4 + (place - 832) // QUARTER,
                    ),
                ),
            ),
        )
        here = group * GROUP_BLOCKS + rel
        held = (here >= 0) & (here < total_blocks)
        late = place - windows_end
        slot_row = late % COARSE_SLOT
        coarse_block = late // COARSE_SLOT * GROUP_BLOCKS + slot_row * POOL // BLOCK
        apart = jnp.abs(coarse_block - (group * GROUP_BLOCKS + block)) > FAR_REACH
        allowed = ((place < windows_end) & held) | (
            (place >= windows_end) & (slot_row < COARSE_USED) & apart
        )
        log_size = jnp.where(
            place < 384, 0.0, jnp.where(place < 640, 1.0, jnp.where(place < windows_end, 2.0, math.log2(POOL)))
        )
        bias[pl.ds(block, 1), :] = jnp.where(allowed, log_size, -jnp.inf)

    def gather(chunk):
        for kind in (KIND_K, KIND_V):
            own_copy(kind, chunk).wait()
            exchange(kind, chunk).wait_recv()
        start_routes(FIRST_HOP[:2], chunk)
        slot = pl.ds(pl.multiple_of(group * COARSE_SLOT, COARSE_SLOT), COARSE_SLOT)
        for side in range(2):
            rows = fine[chunk, side, BLOCK : BLOCK + GROUP_ROWS]
            twos = pooled(rows, GROUP_ROWS // 2, 2)
            fours = pooled(twos, GROUP_ROWS // 4, 2)
            mid[chunk, side, -MID_LOW * HALF : (GROUP_BLOCKS - MID_LOW) * HALF] = twos
            far[chunk, side, -FAR_LOW * QUARTER : (GROUP_BLOCKS - FAR_LOW) * QUARTER] = fours
            coarse[chunk, side, slot] = pooled(fours, COARSE_SLOT, POOL // 4)
        start_routes(FIRST_HOP[2:], chunk)

        @pl.loop(1, groups)
        def _(step):
            coarse_copy(chunk, step).start()

    def relay(chunk):
        await_routes(FIRST_HOP, chunk)
        for side in range(2):
            mid[chunk, side, 2 * HALF : 3 * HALF] = pooled(fine[chunk, side, :BLOCK], HALF, 2)
            mid[chunk, side, 7 * HALF : 8 * HALF] = pooled(fine[chunk, side, 5 * BLOCK :], HALF, 2)
            far[chunk, side, 6 * QUARTER : 9 * QUARTER] = pooled(
                mid[chunk, side, : 3 * HALF], 3 * QUARTER, 2
            )
            far[chunk, side, 13 * QUARTER : 16 * QUARTER] = pooled(
                mid[chunk, side, 7 * HALF :], 3 * QUARTER, 2
            )
        start_routes(SECOND_HOP, chunk)

    def forward(chunk):
        await_routes(SECOND_HOP, chunk)
        start_routes(THIRD_HOP, chunk)

    scale = math.log2(math.e) / math.sqrt(HEAD_DIM)

    def attend(chunk):
        own_copy(KIND_Q, chunk).wait()
        exchange(KIND_Q, chunk).wait_recv()
        await_routes(THIRD_HOP, chunk)

        @pl.loop(1, groups)
        def _(step):
            origin = pl.ds(
                pl.multiple_of(lax.rem(group - step + groups, groups) * COARSE_SLOT, COARSE_SLOT), COARSE_SLOT
            )
            pltpu.make_async_remote_copy(
                src_ref=coarse.at[chunk, :, origin], dst_ref=coarse.at[chunk, :, origin],
                send_sem=coarse_send.at[chunk, step], recv_sem=coarse_recv.at[chunk, step],
                device_id={"seq": partner}, device_id_type=MESH,
            ).wait_recv()

        for block in range(GROUP_BLOCKS):
            def atom_rows(side):
                return jnp.concatenate(
                    [
                        fine[chunk, side, block * BLOCK : (block + 3) * BLOCK],
                        mid[chunk, side, block * HALF : (block + 2) * HALF],
                        mid[chunk, side, (block + 5) * HALF : (block + 7) * HALF],
                        far[chunk, side, block * QUARTER : (block + 6) * QUARTER],
                        far[chunk, side, (block + 13) * QUARTER : (block + 19) * QUARTER],
                        coarse[chunk, side],
                    ],
                    axis=0,
                )

            scores = lax.dot_general(
                q_rows[chunk, block * BLOCK : (block + 1) * BLOCK], atom_rows(0),
                (((1,), (1,)), ((), ())), preferred_element_type=jnp.float32,
            ) * scale + bias[pl.ds(block, 1), :]
            row_top = jnp.max(scores, axis=1, keepdims=True)
            exp_terms = jnp.exp2(scores - row_top)
            denominator = jnp.sum(exp_terms, axis=1, keepdims=True)
            weighted = jnp.dot(
                exp_terms.astype(jnp.bfloat16), atom_rows(1), preferred_element_type=jnp.float32
            )
            out_rows[chunk, block * BLOCK : (block + 1) * BLOCK] = (weighted / denominator).astype(
                jnp.bfloat16
            )
        exchange(KIND_O, chunk).start()
        own_result(chunk).start()

    stages = ((gather, 0), (relay, RELAY_LAG), (forward, FORWARD_LAG), (attend, ATTEND_LAG))

    @pl.loop(0, chunks + ATTEND_LAG)
    def _(step):
        for stage, lag in stages:
            @pl.when((step >= lag) & (step < chunks + lag))
            def _():
                stage(step - lag)

    @pl.loop(0, chunks)
    def _(chunk):
        own_result(chunk).wait()
        exchange(KIND_O, chunk).wait_recv()
        for kind in (KIND_K, KIND_V, KIND_Q, KIND_O):
            exchange(kind, chunk).wait_send()
        for route in ROUTES:
            hop = hop_of(route[1])

            @pl.when(inside(hop) & inside(hop - route[1]))
            def _():
                routed(route, chunk).wait_send()

        @pl.loop(1, groups)
        def _(step):
            coarse_copy(chunk, step).wait_send()


def per_device(queries, key_rows, value_rows):
    rows_dev, cols = queries.shape
    groups = lax.axis_size("seq") // 2
    chunks = cols // 2 // HEAD_DIM
    atoms = 8 * BLOCK + groups * COARSE_SLOT
    bf16 = jnp.bfloat16
    placed = pl.BlockSpec(memory_space=pltpu.HBM)
    return pl.pallas_call(
        functools.partial(kernel, groups),
        out_shape=jax.ShapeDtypeStruct(queries.shape, bf16),
        in_specs=[placed] * 3,
        out_specs=placed,
        scratch_shapes=[
            pltpu.VMEM((chunks, 2 * rows_dev, HEAD_DIM), bf16),
            pltpu.VMEM((chunks, 2, FINE_BLOCKS * BLOCK, HEAD_DIM), bf16),
            pltpu.VMEM((chunks, 2, MID_BLOCKS * HALF, HEAD_DIM), bf16),
            pltpu.VMEM((chunks, 2, FAR_BLOCKS * QUARTER, HEAD_DIM), bf16),
            pltpu.VMEM((chunks, 2, groups * COARSE_SLOT, HEAD_DIM), bf16),
            pltpu.VMEM((chunks, 2 * rows_dev, HEAD_DIM), bf16),
            pltpu.VMEM((8, atoms), jnp.float32),
            pltpu.SemaphoreType.DMA((chunks, KINDS)),
            pltpu.SemaphoreType.DMA((chunks, KINDS)),
            pltpu.SemaphoreType.DMA((chunks, groups)),
            pltpu.SemaphoreType.DMA((chunks, groups)),
            pltpu.SemaphoreType.DMA((chunks, 4)),
        ],
        compiler_params=pltpu.CompilerParams(
            collective_id=0, has_side_effects=True, vmem_limit_bytes=48 * 1024 * 1024
        ),
    )(queries, key_rows, value_rows)


def solution(mesh):
    placed = (P("seq", "head"), P("seq", "head"), P("seq", "head"))
    return jax.shard_map(
        per_device, mesh=mesh, in_specs=placed, out_specs=P("seq", "head"), check_vma=False
    )
```

```python
import functools
import math

import jax
import jax.numpy as jnp
from jax import lax
from jax.experimental import pallas as pl
from jax.experimental.pallas import tpu as pltpu
from jax.sharding import PartitionSpec as P

HEAD_DIM = 128
BLOCK = 128
POOL = 64
MID_REACH = 3
FAR_REACH = 9

HALF = BLOCK // 2
QUARTER = BLOCK // 4
GROUP_BLOCKS = 4
GROUP_ROWS = GROUP_BLOCKS * BLOCK
COARSE_SLOT = 16
COARSE_USED = GROUP_ROWS // POOL

FINE_LOW, FINE_BLOCKS = -1, GROUP_BLOCKS + 2
MID_LOW, MID_BLOCKS = -MID_REACH, GROUP_BLOCKS + 2 * MID_REACH
FAR_LOW, FAR_BLOCKS = -FAR_REACH, GROUP_BLOCKS + 2 * FAR_REACH

KIND_K, KIND_V, KIND_Q, KIND_O = 0, 1, 2, 3
FIRST_HOP = (
    (4, 1, "fine", 3, 1, -1),
    (5, -1, "fine", 0, 1, 4),
    (6, 1, "mid", 1, 2, -3),
    (7, -1, "mid", 1, 2, 5),
    (8, 1, "far", 0, 1, -4),
    (9, -1, "far", 3, 1, 7),
)
SECOND_HOP = (
    (10, 2, "far", -4, 4, -8),
    (11, -2, "far", 4, 4, 8),
)
THIRD_HOP = (
    (12, 3, "far", -5, 1, -9),
    (13, -3, "far", 8, 1, 12),
)
ROUTES = FIRST_HOP + SECOND_HOP + THIRD_HOP
RELAY_LAG, FORWARD_LAG, ATTEND_LAG = 2, 3, 4
KINDS = 14
MESH = pl.DeviceIdType.MESH


def hop_of(offset):
    return 1 if offset > 0 else -1


def pool_matrix(out_rows, in_rows, group_rows):
    row = lax.broadcasted_iota(jnp.int32, (out_rows, in_rows), 0)
    col = lax.broadcasted_iota(jnp.int32, (out_rows, in_rows), 1)
    return jnp.where(col // group_rows == row, 1.0 / group_rows, 0.0).astype(jnp.bfloat16)


def pooled(source, out_rows, group_rows):
    weights = pool_matrix(out_rows, source.shape[0], group_rows)
    return jnp.dot(weights, source, preferred_element_type=jnp.float32).astype(jnp.bfloat16)


def kernel(
    groups, q_ref, k_ref, v_ref, o_ref,
    q_rows, fine, mid, far, coarse, out_rows, bias,
    send, recv, coarse_send, coarse_recv, local,
):
    me = lax.axis_index("seq")
    group = me // 2
    parity = me % 2
    partner = me + 1 - 2 * parity
    rows_dev = q_ref.shape[0]
    chunks = q_rows.shape[0]
    half_cols = chunks * HEAD_DIM
    own_first = pl.multiple_of(parity * rows_dev, rows_dev)
    other_first = pl.multiple_of((1 - parity) * rows_dev, rows_dev)
    levels = {"fine": (fine, BLOCK, FINE_LOW), "mid": (mid, HALF, MID_LOW), "far": (far, QUARTER, FAR_LOW)}

    def own_cols(chunk):
        return pl.ds(pl.multiple_of(parity * half_cols + chunk * HEAD_DIM, HEAD_DIM), HEAD_DIM)

    def other_cols(chunk):
        return pl.ds(pl.multiple_of((1 - parity) * half_cols + chunk * HEAD_DIM, HEAD_DIM), HEAD_DIM)

    def remote(src, dst, kind, chunk, target):
        return pltpu.make_async_remote_copy(
            src_ref=src, dst_ref=dst, send_sem=send.at[chunk, kind], recv_sem=recv.at[chunk, kind],
            device_id={"seq": target}, device_id_type=MESH,
        )

    def exchange(kind, chunk):
        if kind == KIND_Q:
            return remote(
                q_ref.at[:, other_cols(chunk)], q_rows.at[chunk, pl.ds(own_first, rows_dev)],
                kind, chunk, partner,
            )
        if kind == KIND_O:
            return remote(
                out_rows.at[chunk, pl.ds(other_first, rows_dev)], o_ref.at[:, own_cols(chunk)],
                kind, chunk, partner,
            )
        source = k_ref if kind == KIND_K else v_ref
        return remote(
            source.at[:, other_cols(chunk)], fine.at[chunk, kind, pl.ds(BLOCK + own_first, rows_dev)],
            kind, chunk, partner,
        )

    def routed(route, chunk):
        kind, offset, level, first, count, landing = route
        window, unit, low = levels[level]
        return remote(
            window.at[chunk, :, pl.ds((first - low) * unit, count * unit)],
            window.at[chunk, :, pl.ds((landing - low) * unit, count * unit)],
            kind, chunk, me + 2 * hop_of(offset),
        )

    def coarse_copy(chunk, step):
        target = lax.rem(group + step, groups) * 2 + parity
        slot = pl.ds(pl.multiple_of(group * COARSE_SLOT, COARSE_SLOT), COARSE_SLOT)
        return pltpu.make_async_remote_copy(
            src_ref=coarse.at[chunk, :, slot], dst_ref=coarse.at[chunk, :, slot],
            send_sem=coarse_send.at[chunk, step], recv_sem=coarse_recv.at[chunk, step],
            device_id={"seq": target}, device_id_type=MESH,
        )

    def inside(offset):
        return (group + offset >= 0) & (group + offset < groups)

    def start_routes(routes, chunk):
        for route in routes:
            hop = hop_of(route[1])

            @pl.when(inside(hop) & inside(hop - route[1]))
            def _():
                routed(route, chunk).start()

    def await_routes(routes, chunk):
        for route in routes:
            @pl.when(inside(-route[1]))
            def _():
                routed(route, chunk).wait_recv()

    def own_copy(kind, chunk):
        if kind == KIND_Q:
            source, target = q_ref, q_rows.at[chunk, pl.ds(own_first, rows_dev)]
        else:
            source = k_ref if kind == KIND_K else v_ref
            target = fine.at[chunk, kind, pl.ds(BLOCK + own_first, rows_dev)]
        return pltpu.make_async_copy(source.at[:, own_cols(chunk)], target, local.at[chunk, kind])

    def own_result(chunk):
        return pltpu.make_async_copy(
            out_rows.at[chunk, pl.ds(own_first, rows_dev)], o_ref.at[:, own_cols(chunk)],
            local.at[chunk, KIND_O],
        )

    barrier = pltpu.get_barrier_semaphore()
    pl.semaphore_signal(barrier, inc=1, device_id={"seq": partner}, device_id_type=MESH)

    @pl.loop(1, groups)
    def _(step):
        target = lax.rem(group + step, groups) * 2 + parity
        pl.semaphore_signal(barrier, inc=1, device_id={"seq": target}, device_id_type=MESH)

    pl.semaphore_wait(barrier, groups)

    @pl.loop(0, chunks)
    def _(chunk):
        exchange(KIND_K, chunk).start()
        exchange(KIND_V, chunk).start()
        own_copy(KIND_K, chunk).start()
        own_copy(KIND_V, chunk).start()

    @pl.loop(0, chunks)
    def _(chunk):
        exchange(KIND_Q, chunk).start()
        own_copy(KIND_Q, chunk).start()

    for _, offset, level, _, count, landing in ROUTES:
        window, unit, low = levels[level]

        @pl.when(jnp.logical_not(inside(-offset)))
        def _():
            @pl.loop(0, chunks)
            def _(chunk):
                window[chunk, :, pl.ds((landing - low) * unit, count * unit)] = jnp.zeros(
                    (2, count * unit, HEAD_DIM), jnp.bfloat16
                )

    atoms = bias.shape[1]
    total_blocks = groups * GROUP_BLOCKS
    place = lax.broadcasted_iota(jnp.int32, (1, atoms), 1)
    windows_end = 8 * BLOCK
    for block in range(GROUP_BLOCKS):
        rel = jnp.where(
            place < 384,
            block - 1 + place // BLOCK,
            jnp.where(
                place < 512,
                block - 3 + (place - 384) // HALF,
                jnp.where(
                    place < 640,
                    block + 2 + (place - 512) // HALF,
                    jnp.where(
                        place < 832,
                        block - 9 + (place - 640) // QUARTER,
                        block + 4 + (place - 832) // QUARTER,
                    ),
                ),
            ),
        )
        here = group * GROUP_BLOCKS + rel
        held = (here >= 0) & (here < total_blocks)
        late = place - windows_end
        slot_row = late % COARSE_SLOT
        coarse_block = late // COARSE_SLOT * GROUP_BLOCKS + slot_row * POOL // BLOCK
        apart = jnp.abs(coarse_block - (group * GROUP_BLOCKS + block)) > FAR_REACH
        allowed = ((place < windows_end) & held) | (
            (place >= windows_end) & (slot_row < COARSE_USED) & apart
        )
        log_size = jnp.where(
            place < 384, 0.0, jnp.where(place < 640, 1.0, jnp.where(place < windows_end, 2.0, math.log2(POOL)))
        )
        bias[pl.ds(block, 1), :] = jnp.where(allowed, log_size, -jnp.inf)

    def gather(chunk):
        for kind in (KIND_K, KIND_V):
            own_copy(kind, chunk).wait()
            exchange(kind, chunk).wait_recv()
        start_routes(FIRST_HOP[:2], chunk)
        slot = pl.ds(pl.multiple_of(group * COARSE_SLOT, COARSE_SLOT), COARSE_SLOT)
        for side in range(2):
            rows = fine[chunk, side, BLOCK : BLOCK + GROUP_ROWS]
            twos = pooled(rows, GROUP_ROWS // 2, 2)
            fours = pooled(twos, GROUP_ROWS // 4, 2)
            mid[chunk, side, -MID_LOW * HALF : (GROUP_BLOCKS - MID_LOW) * HALF] = twos
            far[chunk, side, -FAR_LOW * QUARTER : (GROUP_BLOCKS - FAR_LOW) * QUARTER] = fours
            coarse[chunk, side, slot] = pooled(fours, COARSE_SLOT, POOL // 4)
        start_routes(FIRST_HOP[2:], chunk)

        @pl.loop(1, groups)
        def _(step):
            @pl.when(jnp.abs(lax.rem(group + step, groups) - group) > 2)
            def _():
                coarse_copy(chunk, step).start()

    def relay(chunk):
        await_routes(FIRST_HOP, chunk)
        for side in range(2):
            mid[chunk, side, 2 * HALF : 3 * HALF] = pooled(fine[chunk, side, :BLOCK], HALF, 2)
            mid[chunk, side, 7 * HALF : 8 * HALF] = pooled(fine[chunk, side, 5 * BLOCK :], HALF, 2)
            far[chunk, side, 6 * QUARTER : 9 * QUARTER] = pooled(
                mid[chunk, side, : 3 * HALF], 3 * QUARTER, 2
            )
            far[chunk, side, 13 * QUARTER : 16 * QUARTER] = pooled(
                mid[chunk, side, 7 * HALF :], 3 * QUARTER, 2
            )
        start_routes(SECOND_HOP, chunk)

    def forward(chunk):
        await_routes(SECOND_HOP, chunk)
        start_routes(THIRD_HOP, chunk)

    scale = math.log2(math.e) / math.sqrt(HEAD_DIM)

    def attend(chunk):
        own_copy(KIND_Q, chunk).wait()
        exchange(KIND_Q, chunk).wait_recv()
        await_routes(THIRD_HOP, chunk)

        @pl.loop(1, groups)
        def _(step):
            giver = lax.rem(group - step + groups, groups)
            origin = pl.ds(pl.multiple_of(giver * COARSE_SLOT, COARSE_SLOT), COARSE_SLOT)

            @pl.when(jnp.abs(giver - group) > 2)
            def _():
                pltpu.make_async_remote_copy(
                    src_ref=coarse.at[chunk, :, origin], dst_ref=coarse.at[chunk, :, origin],
                    send_sem=coarse_send.at[chunk, step], recv_sem=coarse_recv.at[chunk, step],
                    device_id={"seq": partner}, device_id_type=MESH,
                ).wait_recv()

        for offset in (-2, -1, 1, 2):
            @pl.when(inside(offset))
            def _():
                near = pl.ds(pl.multiple_of((group + offset) * COARSE_SLOT, COARSE_SLOT), COARSE_SLOT)
                first = (offset * GROUP_BLOCKS - FAR_LOW) * QUARTER
                for side in range(2):
                    fours = far[chunk, side, first : first + GROUP_ROWS // 4]
                    coarse[chunk, side, near] = pooled(fours, COARSE_SLOT, POOL // 4)

        for block in range(GROUP_BLOCKS):
            def atom_rows(side):
                return jnp.concatenate(
                    [
                        fine[chunk, side, block * BLOCK : (block + 3) * BLOCK],
                        mid[chunk, side, block * HALF : (block + 2) * HALF],
                        mid[chunk, side, (block + 5) * HALF : (block + 7) * HALF],
                        far[chunk, side, block * QUARTER : (block + 6) * QUARTER],
                        far[chunk, side, (block + 13) * QUARTER : (block + 19) * QUARTER],
                        coarse[chunk, side],
                    ],
                    axis=0,
                )

            scores = lax.dot_general(
                q_rows[chunk, block * BLOCK : (block + 1) * BLOCK], atom_rows(0),
                (((1,), (1,)), ((), ())), preferred_element_type=jnp.float32,
            ) * scale + bias[pl.ds(block, 1), :]
            row_top = jnp.max(scores, axis=1, keepdims=True)
            exp_terms = jnp.exp2(scores - row_top)
            denominator = jnp.sum(exp_terms, axis=1, keepdims=True)
            weighted = jnp.dot(
                exp_terms.astype(jnp.bfloat16), atom_rows(1), preferred_element_type=jnp.float32
            )
            out_rows[chunk, block * BLOCK : (block + 1) * BLOCK] = (weighted / denominator).astype(
                jnp.bfloat16
            )
        exchange(KIND_O, chunk).start()
        own_result(chunk).start()

    stages = ((gather, 0), (relay, RELAY_LAG), (forward, FORWARD_LAG), (attend, ATTEND_LAG))

    @pl.loop(0, chunks + ATTEND_LAG)
    def _(step):
        for stage, lag in stages:
            @pl.when((step >= lag) & (step < chunks + lag))
            def _():
                stage(step - lag)

    @pl.loop(0, chunks)
    def _(chunk):
        own_result(chunk).wait()
        exchange(KIND_O, chunk).wait_recv()
        for kind in (KIND_K, KIND_V, KIND_Q, KIND_O):
            exchange(kind, chunk).wait_send()
        for route in ROUTES:
            hop = hop_of(route[1])

            @pl.when(inside(hop) & inside(hop - route[1]))
            def _():
                routed(route, chunk).wait_send()

        @pl.loop(1, groups)
        def _(step):
            @pl.when(jnp.abs(lax.rem(group + step, groups) - group) > 2)
            def _():
                coarse_copy(chunk, step).wait_send()


def per_device(queries, key_rows, value_rows):
    rows_dev, cols = queries.shape
    groups = lax.axis_size("seq") // 2
    chunks = cols // 2 // HEAD_DIM
    atoms = 8 * BLOCK + groups * COARSE_SLOT
    bf16 = jnp.bfloat16
    placed = pl.BlockSpec(memory_space=pltpu.HBM)
    return pl.pallas_call(
        functools.partial(kernel, groups),
        out_shape=jax.ShapeDtypeStruct(queries.shape, bf16),
        in_specs=[placed] * 3,
        out_specs=placed,
        scratch_shapes=[
            pltpu.VMEM((chunks, 2 * rows_dev, HEAD_DIM), bf16),
            pltpu.VMEM((chunks, 2, FINE_BLOCKS * BLOCK, HEAD_DIM), bf16),
            pltpu.VMEM((chunks, 2, MID_BLOCKS * HALF, HEAD_DIM), bf16),
            pltpu.VMEM((chunks, 2, FAR_BLOCKS * QUARTER, HEAD_DIM), bf16),
            pltpu.VMEM((chunks, 2, groups * COARSE_SLOT, HEAD_DIM), bf16),
            pltpu.VMEM((chunks, 2 * rows_dev, HEAD_DIM), bf16),
            pltpu.VMEM((8, atoms), jnp.float32),
            pltpu.SemaphoreType.DMA((chunks, KINDS)),
            pltpu.SemaphoreType.DMA((chunks, KINDS)),
            pltpu.SemaphoreType.DMA((chunks, groups)),
            pltpu.SemaphoreType.DMA((chunks, groups)),
            pltpu.SemaphoreType.DMA((chunks, 4)),
        ],
        compiler_params=pltpu.CompilerParams(
            collective_id=0, has_side_effects=True, vmem_limit_bytes=48 * 1024 * 1024
        ),
    )(queries, key_rows, value_rows)


def solution(mesh):
    placed = (P("seq", "head"), P("seq", "head"), P("seq", "head"))
    return jax.shard_map(
        per_device, mesh=mesh, in_specs=placed, out_specs=P("seq", "head"), check_vma=False
    )
```
